32 devices in a mesh: groups: 2 (over y), seq: 16 (over z, x, core).
Axes of the slice: x: 2, y: 2, z: 4, core: 2. Of those that a mesh axis runs over, the one named last changes fastest.
Arguments:
- queries: bfloat16 [8192, 2048], P(('groups', 'seq')), parts along dimension 0, may hold values from -20 to 20
- keys: bfloat16 [8192, 2048], P(('groups', 'seq')), parts along dimension 0, may hold values from -20 to 20
- values: bfloat16 [8192, 2048], P(('groups', 'seq')), parts along dimension 0, may hold values from -6 to 6
- block_counts: int32 [16], P('groups'), parts along dimension 0, may hold values from 2 to 6, as said below
- last_tokens: int32 [32], P('groups'), parts along dimension 0, may hold values from 64 to 128
- pack_order: int32 [32], P('groups'), parts along dimension 0, may hold values from 0 to 15, as said below
- decode_slot: int32 [16], P('groups'), parts along dimension 0, may hold values from 0 to 7, each once
Outputs:
- attended: bfloat16 [8192, 2048], P(('groups', 'seq')), parts along dimension 0
- cache_keys: bfloat16 [32, 32, 128, 128], P(('groups', 'seq')), parts along dimension 0
- cache_values: bfloat16 [32, 32, 128, 128], P(('groups', 'seq')), parts along dimension 0
The draws below stay inside these ranges and needn't reach their ends.
There are 2 independent parts, one for each index of `groups`. The reference program is written for one: setup_inputs(seed, part) draws one part's arguments, and reference() takes and returns one part's arrays. A program takes and returns all parts, laid end to end along the dimension named above; each array names one. Nothing has to cross between parts.
Inputs may be any that keep to these rules, and one draw needn't show every extreme that they name: `block_counts`: they sum to 24; the largest equals 6. `pack_order`: each prompt number appears once. The last 1 positions hold null prompts, and the position before them a conditional prompt of 6 blocks. `decode_slot`: each slot appears once.
All inputs are finite; a program needn't handle non-finite values.
Results may differ from the reference program's by a relative error of at most 0.0034.
Values may be sent and summed in bfloat16 or wider, within the bound.
A program may use at most 64 MiB of HBM per device.

```python
import jax
import jax.numpy as jnp
from jax import lax

HEADS = 16
HEAD_DIM = 128
BLOCK = 128
MAXB = 6
BLK_DEV = 2
NB = 32
TOKENS = 4096
PAIRS = 8
SPLITS = 1
SLICE = 128


def draw_queries(key, part):
    noise = jnp.clip(jax.random.normal(jax.random.fold_in(key, 1), (TOKENS, HEADS * HEAD_DIM), jnp.float32), -6.0, 6.0)
    return noise.astype(jnp.bfloat16)


def draw_keys(key, part):
    noise = jnp.clip(jax.random.normal(jax.random.fold_in(key, 2), (TOKENS, HEADS * HEAD_DIM), jnp.float32), -6.0, 6.0)
    return noise.astype(jnp.bfloat16)


def pack_plan(key):
    base = jax.random.fold_in(key, 11)
    first_key, second_key, third_key, fourth_key = jax.random.split(base, 4)
    pair_ids = jnp.arange(PAIRS, dtype=jnp.int32)
    biggest = jax.random.randint(first_key, (), 0, PAIRS).astype(jnp.int32)
    counts = jnp.where(pair_ids == biggest, MAXB, 2).astype(jnp.int32)
    extra = NB - PAIRS - (2 * (PAIRS - 1) + MAXB)

    def add_one(step, current):
        scores = jax.random.randint(jax.random.fold_in(second_key, step), (PAIRS,), 0, 1 << 20).astype(jnp.int32) * PAIRS + pair_ids
        scores = jnp.where(current < MAXB, scores, -1)
        chosen = jnp.argmax(scores).astype(jnp.int32)
        return current + (pair_ids == chosen).astype(jnp.int32)
    counts = lax.fori_loop(0, extra, add_one, counts)
    null_order = jax.random.permutation(third_key, PAIRS).astype(jnp.int32)
    tail_nulls = PAIRS + null_order[:BLK_DEV - 1]
    spare_nulls = PAIRS + null_order[BLK_DEV - 1:]
    spare_count = PAIRS - BLK_DEV + 1
    cond_order = jax.random.permutation(fourth_key, PAIRS).astype(jnp.int32)
    rank_keys = jnp.where(cond_order == biggest, PAIRS, pair_ids).astype(jnp.int32)
    cond_seq = cond_order[jnp.argsort(rank_keys, stable=True)][:PAIRS - 1]
    first_edge = BLK_DEV
    middle_edge = NB // BLK_DEV // 2 * BLK_DEV
    order = jnp.zeros((2 * PAIRS,), jnp.int32)

    def place(step, carry):
        current, write, start, queue = carry
        prompt = cond_seq[step]
        size = counts[prompt]
        filler = (start + size == first_edge) | (start + size == middle_edge)
        current = current.at[write].set(jnp.where(filler, spare_nulls[queue], prompt))
        bump = filler.astype(jnp.int32)
        write = write + bump
        start = start + bump
        queue = queue + bump
        current = current.at[write].set(prompt)
        return (current, write + 1, start + size, queue)
    zero = jnp.zeros((), jnp.int32)
    order, write, start, queue = lax.fori_loop(0, PAIRS - 1, place, (order, zero, zero, zero))

    def rest(index, current):
        keep = index >= queue
        target = jnp.where(keep, write + index - queue, 2 * PAIRS - 1).astype(jnp.int32)
        return current.at[target].set(jnp.where(keep, spare_nulls[index], current[target]))
    order = lax.fori_loop(0, spare_count, rest, order)
    order = order.at[2 * PAIRS - BLK_DEV].set(biggest)
    order = order.at[2 * PAIRS - BLK_DEV + 1:].set(tail_nulls)
    return (counts, order.astype(jnp.int32))


def draw_block_counts(key, part):
    counts, order = pack_plan(key)
    return counts


def draw_pack_order(key, part):
    counts, order = pack_plan(key)
    return order


def touch_ends(array, rng, smallest, high):
    shape = array.shape
    spot = [jax.random.randint(jax.random.fold_in(rng, axis), (), 0, shape[axis]) for axis in range(len(shape))]
    array = array.at[tuple(spot)].set(smallest)
    longest = shape.index(max(shape))
    spot[longest] = (spot[longest] + 1) % shape[longest]
    return array.at[tuple(spot)].set(high)


def levels(rng, shape, cuts, smallest, largest):
    factor_of = 1.0
    for dim, parts in cuts:
        draws = jax.random.uniform(jax.random.fold_in(jax.random.fold_in(rng, 6), dim), (parts,), jnp.float32, smallest / len(cuts), largest / len(cuts))
        factor_of = factor_of * jnp.repeat(jnp.exp(draws), shape[dim] // parts).reshape((-1,) + (1,) * (len(shape) - 1 - dim))
    return factor_of


def bell_draw(rng, shape, scale, reach, cuts=(), kind=jnp.bfloat16):
    factor_of = levels(rng, shape, cuts, -0.22, 0.18) if cuts else 1.0
    array = jax.random.normal(rng, shape, jnp.float32) * scale * factor_of
    return jnp.minimum(jnp.maximum(array, -reach), reach).astype(kind)


def setup_inputs(seed: int = 0, part: int = 0) -> dict:
    splits = jax.random.split(jax.random.key(seed), 8)
    own_keys = jax.random.split(jax.random.fold_in(splits[7], part), 8)
    queries = draw_queries(jax.random.fold_in(jax.random.fold_in(splits[7], part), 71), part)
    keys = draw_keys(jax.random.fold_in(jax.random.fold_in(splits[7], part), 71), part)
    values = bell_draw(own_keys[2], (TOKENS, HEADS * HEAD_DIM), 1.0, 6.0, ((0, 16),))
    block_counts = draw_block_counts(jax.random.fold_in(jax.random.fold_in(splits[7], part), 71), part)
    last_tokens = touch_ends(jax.random.randint(own_keys[4], (2 * PAIRS,), BLOCK // 2, BLOCK + 1), jax.random.fold_in(own_keys[4], 1), BLOCK // 2, BLOCK).astype(jnp.int32)
    pack_order = draw_pack_order(jax.random.fold_in(jax.random.fold_in(splits[7], part), 71), part)
    decode_slot = jax.random.permutation(own_keys[6], PAIRS).astype(jnp.int32)
    return {"queries": queries, "keys": keys, "values": values, "block_counts": block_counts, "last_tokens": last_tokens, "pack_order": pack_order, "decode_slot": decode_slot}


MASKED_SCORE = -1.0e30


def block_tables(block_counts, last_tokens, pack_order, decode_slot, total_blocks, block):
    pair_count = block_counts.shape[0]
    prompts = 2 * pair_count
    prompt_ids = jnp.arange(prompts, dtype=jnp.int32)
    prompt_sizes = jnp.concatenate([block_counts, jnp.ones((pair_count,), jnp.int32)])
    picked = (pack_order[:, None] == prompt_ids[None, :]).astype(jnp.int32)
    packed_sizes = jnp.sum(picked * prompt_sizes[None, :], axis=1).astype(jnp.int32)
    packed_tails = jnp.sum(picked * last_tokens[None, :], axis=1).astype(jnp.int32)
    block_ends = jnp.cumsum(packed_sizes).astype(jnp.int32)
    starts = block_ends - packed_sizes
    blocks = jnp.arange(total_blocks, dtype=jnp.int32)
    member = ((starts[None, :] <= blocks[:, None]) & (blocks[:, None] < block_ends[None, :])).astype(jnp.int32)
    position = jnp.sum(member * prompt_ids[None, :], axis=1).astype(jnp.int32)
    prompt = jnp.sum(member * pack_order[None, :], axis=1).astype(jnp.int32)
    within = blocks - jnp.sum(member * starts[None, :], axis=1).astype(jnp.int32)
    is_last = (blocks + 1) == jnp.sum(member * block_ends[None, :], axis=1).astype(jnp.int32)
    valid_tokens = jnp.where(is_last, jnp.sum(member * packed_tails[None, :], axis=1).astype(jnp.int32), block).astype(jnp.int32)
    pair_ids = jnp.arange(pair_count, dtype=jnp.int32)
    earlier = (decode_slot[None, :] < decode_slot[:, None]).astype(jnp.int32)
    slot_start = jnp.sum(earlier * (block_counts + 1)[None, :], axis=1).astype(jnp.int32)
    pair_of = prompt % pair_count
    owner = (pair_of[:, None] == pair_ids[None, :]).astype(jnp.int32)
    base_slot = jnp.sum(owner * slot_start[None, :], axis=1).astype(jnp.int32)
    own_count = jnp.sum(owner * block_counts[None, :], axis=1).astype(jnp.int32)
    destination = base_slot + jnp.where(prompt >= pair_count, own_count, within)
    hits = (destination[None, :] == blocks[:, None]).astype(jnp.int32)
    source = jnp.sum(hits * blocks[None, :], axis=1).astype(jnp.int32)
    return position, valid_tokens, source


def reference(queries, keys, values, block_counts, last_tokens, pack_order, decode_slot):
    position, valid_tokens, source = block_tables(block_counts, last_tokens, pack_order, decode_slot, NB, BLOCK)
    features = HEADS * HEAD_DIM
    back = MAXB - 1
    span = (back + 1) * BLOCK
    padding = jnp.zeros((back * BLOCK, features), jnp.bfloat16)
    padded_keys = jnp.concatenate([padding, keys], axis=0)
    padded_values = jnp.concatenate([padding, values], axis=0)
    padded_docs = jnp.concatenate([jnp.full((back,), -1, jnp.int32), position])
    padded_valid = jnp.concatenate([jnp.zeros((back,), jnp.int32), valid_tokens])
    token_ids = jnp.arange(BLOCK, dtype=jnp.int32)
    key_blocks = jnp.repeat(jnp.arange(back + 1, dtype=jnp.int32), BLOCK)
    key_tokens = jnp.tile(token_ids, back + 1)
    score_scale = HEAD_DIM ** -0.5

    def one_block(block_index):
        start = (block_index * BLOCK).astype(jnp.int32)
        key_window = lax.dynamic_slice_in_dim(padded_keys, start, span, 0).reshape(span, HEADS, HEAD_DIM)
        value_window = lax.dynamic_slice_in_dim(padded_values, start, span, 0).reshape(span, HEADS, HEAD_DIM)
        window_docs = lax.dynamic_slice_in_dim(padded_docs, block_index, back + 1)
        window_valid = lax.dynamic_slice_in_dim(padded_valid, block_index, back + 1)
        query_block = lax.dynamic_slice_in_dim(queries, start, BLOCK, 0).reshape(BLOCK, HEADS, HEAD_DIM)
        own_doc = window_docs[back]
        own_valid = window_valid[back]
        key_ok = (jnp.repeat(window_docs, BLOCK) == own_doc) & (key_tokens < jnp.repeat(window_valid, BLOCK))
        causal = (key_blocks[None, :] < back) | (key_tokens[None, :] <= token_ids[:, None])
        allowed = causal & key_ok[None, :]
        scores = jnp.einsum("qhd,khd->hqk", query_block.astype(jnp.float32), key_window.astype(jnp.float32)) * score_scale
        scores = jnp.where(allowed[None], scores, MASKED_SCORE)
        peak = jnp.max(scores, axis=2, keepdims=True)
        weights = jnp.exp(scores - peak)
        totals = jnp.sum(weights, axis=2, keepdims=True)
        rounded = lax.optimization_barrier(weights.astype(jnp.bfloat16)).astype(jnp.float32)
        mixed = jnp.einsum("hqk,khd->hqd", rounded, value_window.astype(jnp.float32)) / totals
        mixed = jnp.where((token_ids < own_valid)[None, :, None], mixed, 0.0)
        return jnp.transpose(mixed, (1, 0, 2)).reshape(BLOCK, features).astype(jnp.bfloat16)

    attended = lax.map(one_block, jnp.arange(NB, dtype=jnp.int32)).reshape(TOKENS, features)

    def relayout(source_array):
        grid = source_array.reshape(NB, SPLITS, SLICE, HEADS, HEAD_DIM)
        reordered = jnp.take(grid, source, axis=0)
        return jnp.transpose(reordered, (3, 1, 0, 2, 4)).reshape(HEADS * SPLITS, NB, SLICE, HEAD_DIM)

    return attended, relayout(keys), relayout(values)
```

```python
import functools
import math

import jax
import jax.numpy as jnp
from jax import lax
from jax.experimental import pallas as pl
from jax.experimental.pallas import tpu as pltpu
from jax.sharding import PartitionSpec as P

HEADS = 16
HEAD_DIM = 128
BLOCK = 128
MAXB = 6
BACK = MAXB - 1
HIDDEN = -1e30
PLANE = 4


def window_tables(counts_ref, tails_ref, order_ref, first, width):
    pairs = counts_ref.shape[0]
    prompts = order_ref.shape[0]

    def place(i, carry):
        start, docs, valids = carry
        prompt = order_ref[i]
        counted = counts_ref[lax.rem(prompt, pairs)]
        size = jnp.where(prompt < pairs, counted, 1)
        tail = tails_ref[prompt]
        end = start + size
        new_docs, new_valids = [], []
        for w in range(width):
            b = first + w
            inside = (start <= b) & (b < end)
            new_docs.append(jnp.where(inside, i, docs[w]))
            new_valids.append(
                jnp.where(inside, jnp.where(b + 1 == end, tail, BLOCK), valids[w])
            )
        return end, tuple(new_docs), tuple(new_valids)

    none = jnp.int32(-1)
    zero = jnp.int32(0)
    _, docs, valids = lax.fori_loop(
        0, prompts, place, (zero, (none,) * width, (zero,) * width)
    )
    return docs, valids


def exchange(
    n,
    counts_ref,
    tails_ref,
    order_ref,
    q_ref,
    k_ref,
    v_ref,
    out_ref,
    landed_ref,
    hk,
    hv,
    relay,
    bias,
    halo_send,
    halo_recv,
    relay_recv,
    cache_send,
    cache_recv,
    own_sem,
):
    me = lax.axis_index("seq")
    role = lax.rem(me, PLANE)
    plane = me // PLANE
    planes = n // PLANE
    tokens = q_ref.shape[0]
    here = tokens // BLOCK
    splits = n // HEADS
    part = BLOCK // splits

    barrier = pltpu.get_barrier_semaphore()

    def greet(r, carry):
        pl.semaphore_signal(
            barrier,
            inc=1,
            device_id={"seq": lax.rem(me + r, n)},
            device_id_type=pl.DeviceIdType.MESH,
        )
        return carry

    lax.fori_loop(1, n, greet, 0)
    pl.semaphore_wait(barrier, n - 1)

    own = (k_ref, v_ref)
    halo = (hk, hv)
    pending = []

    def rows(block):
        return pl.ds(block * BLOCK, BLOCK)

    def send(cond, kv, src, target, slot):
        index = len(pending)
        if slot is None:
            dst, recv = relay.at[kv], relay_recv.at[kv]
        else:
            dst, recv = halo[kv].at[rows(slot)], halo_recv.at[kv, slot]
        copy = pltpu.make_async_remote_copy(
            src_ref=src,
            dst_ref=dst,
            send_sem=halo_send.at[index],
            recv_sem=recv,
            device_id={"seq": lax.rem(target + n, n)},
            device_id_type=pl.DeviceIdType.MESH,
        )
        pending.append((cond, copy))
        return copy

    def start(cond, moves):
        copies = [
            send(cond, kv, src(kv), target, slot)
            for src, target, slot in moves
            for kv in range(2)
        ]

        @pl.when(cond)
        def _():
            for copy in copies:
                copy.start()

    def mine(block):
        return lambda kv: own[kv].at[rows(block)]

    def held(slot):
        return lambda kv: halo[kv].at[rows(slot)]

    def await_slots(cond, slots):
        @pl.when(cond)
        def _():
            for slot in slots:
                for kv in range(2):
                    if slot is None:
                        ref, sem = relay.at[kv], relay_recv.at[kv]
                    else:
                        ref, sem = halo[kv].at[rows(slot)], halo_recv.at[kv, slot]
                    pltpu.make_async_copy(ref, ref, sem).wait()

    more = plane < planes - 1
    late = plane > 0
    start((role == 3) & more, [(mine(1), me + 3, 0), (mine(0), me + 3, None)])
    start((role == 2) & more, [(mine(1), me + 2, 2), (mine(0), me + 2, 1)])
    start((role == 1) & more, [(mine(1), me + 3, 0)])
    start(role == 1, [(mine(0), me + 1, 3), (mine(1), me + 1, 4)])
    start(role == 0, [(mine(1), me + 2, 2), (mine(0), me + 2, 1)])
    start(
        (role == 0) | (role == 2), [(mine(0), me + 1, 3), (mine(1), me + 1, 4)]
    )

    def piece(ref, owner, block):
        head = owner // splits
        cols = pl.ds(pl.multiple_of(head * HEAD_DIM, HEAD_DIM), HEAD_DIM)
        if splits == 1:
            return ref.at[:, cols]
        offset = pl.multiple_of(block * BLOCK + lax.rem(owner, splits) * part, part)
        return ref.at[pl.ds(offset, part), cols]

    def place(kv, block):
        if splits == 1:
            return landed_ref.at[kv, pl.ds(pl.multiple_of(me * tokens, tokens), tokens)]
        return landed_ref.at[
            kv, pl.ds(pl.multiple_of((me * here + block) * part, part), part)
        ]

    pieces = 1 if splits == 1 else here

    def give(s, carry):
        sign = 1 - 2 * lax.rem(s, 2)
        target = lax.rem(me + n // 2 + sign * ((s + 1) // 2), n)
        for kv in range(2):
            for block in range(pieces):
                pltpu.make_async_remote_copy(
                    src_ref=piece(own[kv], target, block),
                    dst_ref=place(kv, block),
                    send_sem=cache_send.at[kv],
                    recv_sem=cache_recv.at[kv],
                    device_id={"seq": target},
                    device_id_type=pl.DeviceIdType.MESH,
                ).start()
        return carry

    far = n - 1 - 2 * (PLANE - 1)
    lax.fori_loop(0, far, give, 0)

    await_slots((role == 2) & late, [0, None])
    start(
        (role == 2) & late,
        [(held(0), me - 2 + n, 4), (lambda kv: relay.at[kv], me - 2 + n, 3)],
    )
    await_slots(role == 2, [2, 3, 4])
    start(role == 2, [(held(2), me + 1, 0), (held(3), me + 1, 1), (held(4), me + 1, 2)])
    await_slots((role == 0) & late, [2, 3, 4])
    start(
        (role == 0) & late,
        [(held(2), me + 1, 0), (held(3), me + 1, 1), (held(4), me + 1, 2)],
    )
    lax.fori_loop(far, n - 1, give, 0)
    local = [
        pltpu.make_async_copy(
            piece(own[kv], me, block), place(kv, block), own_sem.at[kv, block]
        )
        for kv in range(2)
        for block in range(pieces)
    ]
    for copy in local:
        copy.start()

    docs, valids = window_tables(
        counts_ref, tails_ref, order_ref, me * here - BACK, BACK + here
    )
    row = lax.broadcasted_iota(jnp.int32, (BLOCK, BLOCK), 0)
    col = lax.broadcasted_iota(jnp.int32, (BLOCK, BLOCK), 1)
    for b in range(here):
        for w in range(BACK + here):
            if w > BACK + b:
                shade = jnp.full((BLOCK, BLOCK), HIDDEN, jnp.float32)
            else:
                limit = jnp.where(docs[w] == docs[BACK + b], valids[w], 0)
                seen = col < limit
                if w == BACK + b:
                    seen = seen & (col <= row)
                shade = jnp.where(seen, 0.0, HIDDEN)
            bias[b * BLOCK : (b + 1) * BLOCK, w * BLOCK : (w + 1) * BLOCK] = shade
    column = lax.broadcasted_iota(jnp.int32, (BLOCK, HEAD_DIM), 0)
    real = jnp.concatenate(
        [column < valids[BACK + b] for b in range(here)], axis=0
    )

    empty = jnp.zeros((BLOCK, hk.shape[1]), hk.dtype)
    for slot, reach in ((0, 3), (1, 2), (2, 2), (3, 1), (4, 1)):

        @pl.when(me < reach)
        def _():
            for kv in range(2):
                halo[kv][slot * BLOCK : (slot + 1) * BLOCK, :] = empty

    await_slots((role == 0) & late, [0, 1])
    await_slots(role == 1, [3, 4])
    await_slots((role == 1) & late, [0, 1, 2])
    await_slots(role == 2, [1])
    await_slots(role == 3, [0, 1, 2, 3, 4])

    factor = HEAD_DIM ** (-0.5) * math.log2(math.e)
    prior = BACK * BLOCK
    nt = (((1,), (1,)), ((), ()))

    def one_head(h, carry):
        cols = pl.ds(pl.multiple_of(h * HEAD_DIM, HEAD_DIM), HEAD_DIM)
        q = q_ref[:, cols]
        s1 = lax.dot_general(q, hk[:, cols], nt, preferred_element_type=jnp.float32)
        s2 = lax.dot_general(q, k_ref[:, cols], nt, preferred_element_type=jnp.float32)
        s1 = s1 + bias[:, :prior]
        s2 = s2 + bias[:, prior:]
        peak = jnp.maximum(
            jnp.max(s1, axis=1, keepdims=True), jnp.max(s2, axis=1, keepdims=True)
        )
        w1 = jnp.exp2((s1 - peak) * factor)
        w2 = jnp.exp2((s2 - peak) * factor)
        total = jnp.sum(w1, axis=1, keepdims=True) + jnp.sum(w2, axis=1, keepdims=True)
        mixed = jnp.dot(
            w1.astype(jnp.bfloat16), hv[:, cols], preferred_element_type=jnp.float32
        ) + jnp.dot(
            w2.astype(jnp.bfloat16), v_ref[:, cols], preferred_element_type=jnp.float32
        )
        out_ref[:, cols] = jnp.where(real, mixed / total, 0.0).astype(out_ref.dtype)
        return carry

    lax.fori_loop(0, HEADS, one_head, 0)

    for cond, copy in pending:

        @pl.when(cond)
        def _():
            copy.wait_send()

    for copy in local:
        copy.wait()
    others = landed_ref.shape[1] // n * (n - 1)
    for kv in range(2):
        ref = landed_ref.at[kv, pl.ds(0, others)]
        pltpu.make_async_copy(ref, ref, cache_send.at[kv]).wait()
        pltpu.make_async_copy(ref, ref, cache_recv.at[kv]).wait()


def reorder(
    counts_ref,
    order_ref,
    slot_ref,
    landed_ref,
    keys_ref,
    values_ref,
    staged,
    who,
    base,
    in_sem,
    out_sem,
):
    pairs = counts_ref.shape[0]
    prompts = order_ref.shape[0]
    blocks, part = staged.shape[1:3]

    def invert(p, carry):
        who[slot_ref[p]] = p
        return carry

    lax.fori_loop(0, pairs, invert, 0)

    def lay(s, first):
        p = who[s]
        base[p] = first
        return first + counts_ref[p] + 1

    lax.fori_loop(0, pairs, lay, jnp.int32(0))

    def fetch(i, first):
        prompt = order_ref[i]
        pair = lax.rem(prompt, pairs)
        null = prompt >= pairs
        counted = counts_ref[pair]
        size = jnp.where(null, 1, counted)
        target = base[pair] + jnp.where(null, counted, 0)

        def one(w, carry):
            for kv in range(2):
                pltpu.make_async_copy(
                    landed_ref.at[kv, pl.ds((first + w) * part, part)],
                    staged.at[kv, target + w],
                    in_sem.at[kv],
                ).start()
            return carry

        lax.fori_loop(0, size, one, 0)
        return first + size

    lax.fori_loop(0, prompts, fetch, jnp.int32(0))
    outs = []
    for kv, ref in enumerate((keys_ref, values_ref)):
        pltpu.make_async_copy(staged.at[kv], staged.at[kv], in_sem.at[kv]).wait()
        copy = pltpu.make_async_copy(staged.at[kv], ref.at[0], out_sem.at[kv])
        copy.start()
        outs.append(copy)
    for copy in outs:
        copy.wait()


def local(n, queries, keys, values, block_counts, last_tokens, pack_order, decode_slot):
    tokens, features = queries.shape
    here = tokens // BLOCK
    splits = n // HEADS
    part = BLOCK // splits
    blocks = here * n
    kind = queries.dtype
    smem = pl.BlockSpec(memory_space=pltpu.SMEM)
    vmem = pl.BlockSpec(memory_space=pltpu.VMEM)
    anywhere = pl.BlockSpec(memory_space=pl.ANY)
    dma = pltpu.SemaphoreType.DMA
    attended, landed = pl.pallas_call(
        functools.partial(exchange, n),
        out_shape=(
            jax.ShapeDtypeStruct((tokens, features), kind),
            jax.ShapeDtypeStruct((2, blocks * part, HEAD_DIM), kind),
        ),
        in_specs=[smem] * 3 + [vmem] * 3,
        out_specs=(vmem, anywhere),
        scratch_shapes=[
            pltpu.VMEM((BACK * BLOCK, features), kind),
            pltpu.VMEM((BACK * BLOCK, features), kind),
            pltpu.VMEM((2, BLOCK, features), kind),
            pltpu.VMEM((tokens, (BACK + here) * BLOCK), jnp.float32),
            dma((64,)),
            dma((2, BACK)),
            dma((2,)),
            dma((2,)),
            dma((2,)),
            dma((2, here)),
        ],
        compiler_params=pltpu.CompilerParams(
            collective_id=0, has_side_effects=True, vmem_limit_bytes=48 * 1024 * 1024
        ),
    )(block_counts, last_tokens, pack_order, queries, keys, values)
    cache = jax.ShapeDtypeStruct((1, blocks, part, HEAD_DIM), kind)
    cache_keys, cache_values = pl.pallas_call(
        reorder,
        out_shape=(cache, cache),
        in_specs=[smem] * 3 + [anywhere],
        out_specs=(anywhere, anywhere),
        scratch_shapes=[
            pltpu.VMEM((2, blocks, part, HEAD_DIM), kind),
            pltpu.SMEM(block_counts.shape, jnp.int32),
            pltpu.SMEM(block_counts.shape, jnp.int32),
            dma((2,)),
            dma((2,)),
        ],
    )(block_counts, pack_order, decode_slot, landed)
    return attended, cache_keys, cache_values


def solution(mesh):
    rows = P(("groups", "seq"), None)
    small = P("groups")
    cache = P(("groups", "seq"), None, None, None)
    return jax.shard_map(
        functools.partial(local, mesh.shape["seq"]),
        mesh=mesh,
        in_specs=(rows, rows, rows, small, small, small, small),
        out_specs=(rows, cache, cache),
        check_vma=False,
    )
```

```python
import functools
import math

import jax
import jax.numpy as jnp
from jax import lax
from jax.experimental import pallas as pl
from jax.experimental.pallas import tpu as pltpu
from jax.sharding import PartitionSpec as P

HEADS = 16
HEAD_DIM = 128
BLOCK = 128
MAXB = 6
BACK = MAXB - 1
HIDDEN = -1e30
PLANE = 4
CHUNKS = 4
RELAY = BACK
ROUND = 2


def window_tables(counts_ref, tails_ref, order_ref, first, width):
    pairs = counts_ref.shape[0]
    prompts = order_ref.shape[0]

    def place(i, carry):
        start, docs, valids = carry
        prompt = order_ref[i]
        counted = counts_ref[lax.rem(prompt, pairs)]
        size = jnp.where(prompt < pairs, counted, 1)
        tail = tails_ref[prompt]
        end = start + size
        new_docs, new_valids = [], []
        for w in range(width):
            b = first + w
            inside = (start <= b) & (b < end)
            new_docs.append(jnp.where(inside, i, docs[w]))
            new_valids.append(
                jnp.where(inside, jnp.where(b + 1 == end, tail, BLOCK), valids[w])
            )
        return end, tuple(new_docs), tuple(new_valids)

    none = jnp.int32(-1)
    zero = jnp.int32(0)
    _, docs, valids = lax.fori_loop(
        0, prompts, place, (zero, (none,) * width, (zero,) * width)
    )
    return docs, valids


def exchange(
    n,
    counts_ref,
    tails_ref,
    order_ref,
    q_hbm,
    k_hbm,
    v_hbm,
    out_ref,
    landed_ref,
    q_ref,
    own,
    halo,
    relay,
    bias,
    halo_send,
    halo_recv,
    cache_sem,
    own_sem,
    load_sem,
):
    me = lax.axis_index("seq")
    role = lax.rem(me, PLANE)
    plane = me // PLANE
    planes = n // PLANE
    tokens, features = q_ref.shape
    here = tokens // BLOCK
    splits = n // HEADS
    part = BLOCK // splits
    wide = features // CHUNKS

    loads = [
        pltpu.make_async_copy(src, dst, load_sem.at[i])
        for i, (src, dst) in enumerate(
            ((k_hbm, own.at[0]), (v_hbm, own.at[1]), (q_hbm, q_ref))
        )
    ]
    for copy in loads:
        copy.start()

    barrier = pltpu.get_barrier_semaphore()

    def greet(r, carry):
        pl.semaphore_signal(
            barrier,
            inc=1,
            device_id={"seq": lax.rem(me + r, n)},
            device_id_type=pl.DeviceIdType.MESH,
        )
        return carry

    lax.fori_loop(1, n, greet, 0)
    loads[0].wait()
    loads[1].wait()
    pl.semaphore_wait(barrier, n - 1)

    pending = []

    def spot(block, c):
        return (
            slice(None),
            pl.ds(block * BLOCK, BLOCK),
            pl.ds(c * wide, wide),
        )

    def mine(block):
        return lambda c: own.at[spot(block, c)]

    def held(slot):
        if slot >= RELAY:
            return lambda c: relay.at[spot(slot - RELAY, c)]
        return lambda c: halo.at[spot(slot, c)]

    def start(cond, c, moves):
        copies = []
        for src, target, slot in moves:
            copy = pltpu.make_async_remote_copy(
                src_ref=src(c),
                dst_ref=held(slot)(c),
                send_sem=halo_send.at[len(pending)],
                recv_sem=halo_recv.at[slot, c],
                device_id={"seq": lax.rem(target + n, n)},
                device_id_type=pl.DeviceIdType.MESH,
            )
            pending.append((cond, copy))
            copies.append(copy)

        @pl.when(cond)
        def _():
            for copy in copies:
                copy.start()

    def await_slots(cond, c, slots):
        @pl.when(cond)
        def _():
            for slot in slots:
                ref = held(slot)(c)
                pltpu.make_async_copy(ref, ref, halo_recv.at[slot, c]).wait()

    more = plane < planes - 1
    late = plane > 0
    for c in range(CHUNKS):
        start((role == 3) & more, c, [(mine(0), me + 3, RELAY), (mine(1), me + 3, 0)])
        if c < ROUND:
            moves = [(mine(1), me - 2, RELAY + 1), (mine(0), me - 2, RELAY)]
        else:
            moves = [(mine(1), me + 2, 2), (mine(0), me + 2, 1)]
        start((role == 2) & more, c, moves)
        start((role == 1) & more, c, [(mine(1), me + 3, 0)])
        start(role == 1, c, [(mine(0), me + 1, 3), (mine(1), me + 1, 4)])
        start(role == 0, c, [(mine(1), me + 2, 2), (mine(0), me + 2, 1)])
        start(
            (role == 0) | (role == 2),
            c,
            [(mine(0), me + 1, 3), (mine(1), me + 1, 4)],
        )

    def piece(owner, block):
        head = owner // splits
        cols = pl.ds(pl.multiple_of(head * HEAD_DIM, HEAD_DIM), HEAD_DIM)
        if splits == 1:
            return own.at[:, :, cols]
        offset = pl.multiple_of(block * BLOCK + lax.rem(owner, splits) * part, part)
        return own.at[:, pl.ds(offset, part), cols]

    def place(block):
        if splits == 1:
            return landed_ref.at[:, pl.ds(pl.multiple_of(me * tokens, tokens), tokens)]
        return landed_ref.at[
            :, pl.ds(pl.multiple_of((me * here + block) * part, part), part)
        ]

    pieces = 1 if splits == 1 else here

    def give(s, carry):
        sign = 1 - 2 * lax.rem(s, 2)
        target = lax.rem(me + n // 2 + sign * ((s + 1) // 2), n)
        for block in range(pieces):
            pltpu.make_async_remote_copy(
                src_ref=piece(target, block),
                dst_ref=place(block),
                send_sem=cache_sem.at[0],
                recv_sem=cache_sem.at[1],
                device_id={"seq": target},
                device_id_type=pl.DeviceIdType.MESH,
            ).start()
        return carry

    cuts = [(n - 1) * i // CHUNKS for i in range(CHUNKS + 1)]

    docs, valids = window_tables(
        counts_ref, tails_ref, order_ref, me * here - BACK, BACK + here
    )
    row = lax.broadcasted_iota(jnp.int32, (BLOCK, BLOCK), 0)
    col = lax.broadcasted_iota(jnp.int32, (BLOCK, BLOCK), 1)
    for b in range(here):
        for w in range(BACK + here):
            if w > BACK + b:
                shade = jnp.full((BLOCK, BLOCK), HIDDEN, jnp.float32)
            else:
                limit = jnp.where(docs[w] == docs[BACK + b], valids[w], 0)
                seen = col < limit
                if w == BACK + b:
                    seen = seen & (col <= row)
                shade = jnp.where(seen, 0.0, HIDDEN)
            bias[b * BLOCK : (b + 1) * BLOCK, w * BLOCK : (w + 1) * BLOCK] = shade
    column = lax.broadcasted_iota(jnp.int32, (BLOCK, HEAD_DIM), 0)
    real = jnp.concatenate(
        [column < valids[BACK + b] for b in range(here)], axis=0
    )

    empty = jnp.zeros((BLOCK, features), halo.dtype)
    for slot, reach in ((0, 3), (1, 2), (2, 2), (3, 1), (4, 1)):

        @pl.when(me < reach)
        def _():
            for kv in range(2):
                halo[kv, slot * BLOCK : (slot + 1) * BLOCK, :] = empty

    loads[2].wait()

    factor = HEAD_DIM ** (-0.5) * math.log2(math.e)
    prior = BACK * BLOCK
    nt = (((1,), (1,)), ((), ()))

    def one_head(h, carry):
        cols = pl.ds(pl.multiple_of(h * HEAD_DIM, HEAD_DIM), HEAD_DIM)
        q = q_ref[:, cols]
        s1 = lax.dot_general(q, halo[0, :, cols], nt, preferred_element_type=jnp.float32)
        s2 = lax.dot_general(q, own[0, :, cols], nt, preferred_element_type=jnp.float32)
        s1 = s1 + bias[:, :prior]
        s2 = s2 + bias[:, prior:]
        peak = jnp.maximum(
            jnp.max(s1, axis=1, keepdims=True), jnp.max(s2, axis=1, keepdims=True)
        )
        w1 = jnp.exp2((s1 - peak) * factor)
        w2 = jnp.exp2((s2 - peak) * factor)
        total = jnp.sum(w1, axis=1, keepdims=True) + jnp.sum(w2, axis=1, keepdims=True)
        mixed = jnp.dot(
            w1.astype(jnp.bfloat16), halo[1, :, cols], preferred_element_type=jnp.float32
        ) + jnp.dot(
            w2.astype(jnp.bfloat16), own[1, :, cols], preferred_element_type=jnp.float32
        )
        out_ref[:, cols] = jnp.where(real, mixed / total, 0.0).astype(out_ref.dtype)
        return carry

    for c in range(CHUNKS):
        lax.fori_loop(cuts[c], cuts[c + 1], give, 0)
        if c < ROUND:
            await_slots((role == 0) & more, c, [RELAY, RELAY + 1])
            start(
                (role == 0) & more,
                c,
                [(held(RELAY + 1), me + PLANE, 2), (held(RELAY), me + PLANE, 1)],
            )
        await_slots((role == 2) & late, c, [RELAY, 0])
        start(
            (role == 2) & late, c, [(held(RELAY), me - 2 + n, 3), (held(0), me - 2 + n, 4)]
        )
        await_slots((role == 0) & late, c, [2, 3, 4])
        await_slots(role == 2, c, [2, 3, 4])
        start(
            (role == 2) | ((role == 0) & late),
            c,
            [(held(2), me + 1, 0), (held(3), me + 1, 1), (held(4), me + 1, 2)],
        )
        await_slots((role == 0) & late, c, [0, 1])
        await_slots(role == 1, c, [3, 4])
        await_slots((role == 1) & late, c, [0, 1, 2])
        await_slots(role == 2, c, [1])
        await_slots(role == 3, c, [0, 1, 2, 3, 4])
        each = HEADS // CHUNKS
        lax.fori_loop(c * each, (c + 1) * each, one_head, 0)

    copies = [
        pltpu.make_async_copy(piece(me, block), place(block), own_sem.at[block])
        for block in range(pieces)
    ]
    for copy in copies:
        copy.start()

    for cond, copy in pending:

        @pl.when(cond)
        def _():
            copy.wait_send()

    for copy in copies:
        copy.wait()
    others = landed_ref.shape[1] // n * (n - 1)
    ref = landed_ref.at[:, pl.ds(0, others)]
    pltpu.make_async_copy(ref, ref, cache_sem.at[0]).wait()
    pltpu.make_async_copy(ref, ref, cache_sem.at[1]).wait()


def reorder(
    counts_ref,
    order_ref,
    slot_ref,
    landed_ref,
    keys_ref,
    values_ref,
    staged,
    who,
    base,
    in_sem,
    out_sem,
):
    pairs = counts_ref.shape[0]
    prompts = order_ref.shape[0]
    blocks, part = staged.shape[1:3]

    def invert(p, carry):
        who[slot_ref[p]] = p
        return carry

    lax.fori_loop(0, pairs, invert, 0)

    def lay(s, first):
        p = who[s]
        base[p] = first
        return first + counts_ref[p] + 1

    lax.fori_loop(0, pairs, lay, jnp.int32(0))

    def fetch(i, first):
        prompt = order_ref[i]
        pair = lax.rem(prompt, pairs)
        null = prompt >= pairs
        counted = counts_ref[pair]
        size = jnp.where(null, 1, counted)
        target = base[pair] + jnp.where(null, counted, 0)

        def one(w, carry):
            for kv in range(2):
                pltpu.make_async_copy(
                    landed_ref.at[kv, pl.ds((first + w) * part, part)],
                    staged.at[kv, target + w],
                    in_sem.at[kv],
                ).start()
            return carry

        lax.fori_loop(0, size, one, 0)
        return first + size

    lax.fori_loop(0, prompts, fetch, jnp.int32(0))
    outs = []
    for kv, ref in enumerate((keys_ref, values_ref)):
        pltpu.make_async_copy(staged.at[kv], staged.at[kv], in_sem.at[kv]).wait()
        copy = pltpu.make_async_copy(staged.at[kv], ref.at[0], out_sem.at[kv])
        copy.start()
        outs.append(copy)
    for copy in outs:
        copy.wait()


def local(n, queries, keys, values, block_counts, last_tokens, pack_order, decode_slot):
    tokens, features = queries.shape
    here = tokens // BLOCK
    splits = n // HEADS
    part = BLOCK // splits
    blocks = here * n
    kind = queries.dtype
    smem = pl.BlockSpec(memory_space=pltpu.SMEM)
    vmem = pl.BlockSpec(memory_space=pltpu.VMEM)
    anywhere = pl.BlockSpec(memory_space=pl.ANY)
    dma = pltpu.SemaphoreType.DMA
    attended, landed = pl.pallas_call(
        functools.partial(exchange, n),
        out_shape=(
            jax.ShapeDtypeStruct((tokens, features), kind),
            jax.ShapeDtypeStruct((2, blocks * part, HEAD_DIM), kind),
        ),
        in_specs=[smem] * 3 + [anywhere] * 3,
        out_specs=(vmem, anywhere),
        scratch_shapes=[
            pltpu.VMEM((tokens, features), kind),
            pltpu.VMEM((2, tokens, features), kind),
            pltpu.VMEM((2, BACK * BLOCK, features), kind),
            pltpu.VMEM((2, 2 * BLOCK, features), kind),
            pltpu.VMEM((tokens, (BACK + here) * BLOCK), jnp.float32),
            dma((CHUNKS * 18,)),
            dma((BACK + 2, CHUNKS)),
            dma((2,)),
            dma((here,)),
            dma((3,)),
        ],
        compiler_params=pltpu.CompilerParams(
            collective_id=0, has_side_effects=True, vmem_limit_bytes=60 * 1024 * 1024
        ),
    )(block_counts, last_tokens, pack_order, queries, keys, values)
    cache = jax.ShapeDtypeStruct((1, blocks, part, HEAD_DIM), kind)
    cache_keys, cache_values = pl.pallas_call(
        reorder,
        out_shape=(cache, cache),
        in_specs=[smem] * 3 + [anywhere],
        out_specs=(anywhere, anywhere),
        scratch_shapes=[
            pltpu.VMEM((2, blocks, part, HEAD_DIM), kind),
            pltpu.SMEM(block_counts.shape, jnp.int32),
            pltpu.SMEM(block_counts.shape, jnp.int32),
            dma((2,)),
            dma((2,)),
        ],
    )(block_counts, pack_order, decode_slot, landed)
    return attended, cache_keys, cache_values


def solution(mesh):
    rows = P(("groups", "seq"), None)
    small = P("groups")
    cache = P(("groups", "seq"), None, None, None)
    return jax.shard_map(
        functools.partial(local, mesh.shape["seq"]),
        mesh=mesh,
        in_specs=(rows, rows, rows, small, small, small, small),
        out_specs=(rows, cache, cache),
        check_vma=False,
    )
```
